128 devices in a mesh: seq: 8 (over x_lo, z), tp: 8 (over y, core), roll: 2 (over x_hi).
Axes of the slice: x: 4 (x_hi: 2, x_lo: 2; x = x_hi * 2 + x_lo), y: 4, z: 4, core: 2. Of those that a mesh axis runs over, the one named last changes fastest.
Arguments:
- hidden: bfloat16 [8, 3584], P('roll'), may hold values from -6 to 6
- norm_gain: bfloat16 [3584], replicated, may hold values from 0.25 to 1.75
- qkv_bias: bfloat16 [3072], replicated, may hold values from -20 to 20
- qkv_weight: bfloat16 [3584, 3072], P(('seq', 'tp', 'roll')), may hold values from -0.09375 to 0.09375
- out_weight: bfloat16 [3584, 2048], P(('seq', 'tp', 'roll')), may hold values from -0.125 to 0.125
- key_cache: bfloat16 [8, 65536, 512], P('roll', ('seq', 'tp')), may hold values from -16 to 16
- value_cache: bfloat16 [8, 65536, 512], P('roll', ('seq', 'tp')), may hold values from -16 to 16
- cache_len: int32 [8], P('roll'), may hold values from 32768 to 65536, as said below
- block_pos: int32 [8, 128], P('roll', ('seq', 'tp')), may hold values from 0 to 16383, as said below
Outputs:
- attended: bfloat16 [8, 3584], P('roll')
- fresh_kv: bfloat16 [8, 1024], P('roll')
- served_qkv: bfloat16 [3584, 4096], P(None, 'tp')
- served_out: bfloat16 [3584, 2048], P(None, 'tp')
The draws below stay inside these ranges and needn't reach their ends.
Inputs may be any that keep to these rules, and one draw needn't show every extreme that they name: `cache_len`: in every draw one rollout has all 65536 positions cached. With i = cache_len[r] mod 8192, and c the 8192-position stretch that holds position cache_len[r]: block_pos[r, b] is i where block b lies in c, i + 8192 where it lies in a later stretch or in the stretch just before c, and 16383 elsewhere.
All inputs are finite; a program needn't handle non-finite values.
Results may differ from the reference program's by a relative error of at most 0.009.
Values may be sent and summed in bfloat16 or wider, within the bound.
No kernel may reach another device: no remote copies, remote signals or barrier semaphores. Data moves between devices by JAX's collectives and lax.ppermute only.
A program may use at most 128 MiB of HBM per device.

```python
import jax
import jax.numpy as jnp
import numpy as np
from jax import lax

D = 3584
HQ = 16
KVH = 4
HD = 128
QKV = 3072
SCOLS = 512
ROLLS = 8
LEN = 65536
BLOCK = 512
NBLK = 128
STRETCH = 8192
N_TP = 8


def shared_lengths(key):
    base_draw = jax.random.randint(jax.random.fold_in(key, 11), (ROLLS,), LEN // 2, LEN + 1)
    chosen = jax.random.randint(jax.random.fold_in(key, 12), (), 0, ROLLS)
    return jnp.where(jnp.arange(ROLLS) == chosen, LEN, base_draw).astype(jnp.int32)


def draw_cache_len(key, part):
    return shared_lengths(key)


def draw_block_pos(key, part):
    lengths = shared_lengths(key)
    block_stretch = jnp.arange(NBLK, dtype=jnp.int32) * BLOCK // STRETCH
    query_stretch = (lengths // STRETCH)[:, None]
    intra_pos = (lengths % STRETCH)[:, None]
    near_pos = jnp.where(block_stretch[None, :] == query_stretch, intra_pos, intra_pos + STRETCH)
    return jnp.where(block_stretch[None, :] >= query_stretch - 1, near_pos, 2 * STRETCH - 1).astype(jnp.int32)


def draw_qkv_bias(key, part):
    bias_draw = 0.5 * jax.random.normal(jax.random.fold_in(key, 31), (QKV,), jnp.float32)
    return jnp.clip(bias_draw, -20.0, 20.0).astype(jnp.bfloat16)


def draw_key_cache(key, part):
    col_total = KVH * HD
    noise_part = jax.random.normal(jax.random.fold_in(key, 41), (ROLLS, NBLK, BLOCK, col_total), jnp.float32)
    region_mean = jax.random.normal(jax.random.fold_in(key, 42), (ROLLS, NBLK, 1, col_total), jnp.float32)
    cached = (noise_part + 0.5 * region_mean).reshape(ROLLS, LEN, col_total)
    return jnp.clip(cached, -16.0, 16.0).astype(jnp.bfloat16)


def draw_value_cache(key, part):
    col_total = KVH * HD
    region_mean = jax.random.normal(jax.random.fold_in(key, 52), (ROLLS, NBLK, 1, col_total), jnp.float32)
    noise_part = jax.random.normal(jax.random.fold_in(key, 51), (ROLLS, NBLK, BLOCK, col_total), jnp.float32)
    cached = noise_part + 2.0 * region_mean
    return jnp.clip(cached.reshape(ROLLS, LEN, col_total), -16.0, 16.0).astype(jnp.bfloat16)


def level_of(key, extent, cuts, smallest, largest):
    gain, own = 1.0, jax.random.fold_in(key, 6)
    for dim, shards_of in cuts:
        steps = jnp.exp(jax.random.uniform(jax.random.fold_in(own, dim), (shards_of,), jnp.float32, smallest / len(cuts), largest / len(cuts)))
        gain = gain * jnp.repeat(steps, extent[dim] // shards_of).reshape([-1 if axis == dim else 1 for axis in range(len(extent))])
    return gain


def centred(rng, dims, deviation, bound, pieces=(), kind=jnp.bfloat16):
    values = jax.random.normal(rng, dims, jnp.float32) * deviation
    if len(pieces) > 0:
        values = level_of(rng, dims, pieces, -0.22, 0.18) * values
    return jnp.clip(values, min=-bound, max=bound).astype(kind)


def setup_inputs(seed: int = 0) -> dict:
    keys = jax.random.split(jax.random.key(seed), 10)
    return {
        "hidden": centred(keys[0], (ROLLS, D), 1.0, 6.0, ((0, 2),)),
        "norm_gain": jnp.clip(1.0 + 0.15 * jax.random.normal(keys[1], (D,), jnp.float32), 0.25, 1.75).astype(jnp.bfloat16),
        "qkv_bias": draw_qkv_bias(jax.random.fold_in(keys[9], 71), 0),
        "qkv_weight": centred(keys[3], (D, QKV), D ** -0.5, 0.09375, ((0, 128),)),
        "out_weight": centred(keys[4], (D, HQ * HD), (HQ * HD) ** -0.5, 0.125, ((0, 128),)),
        "key_cache": draw_key_cache(jax.random.fold_in(keys[9], 71), 0),
        "value_cache": draw_value_cache(jax.random.fold_in(keys[9], 71), 0),
        "cache_len": draw_cache_len(jax.random.fold_in(keys[9], 71), 0),
        "block_pos": draw_block_pos(jax.random.fold_in(keys[9], 71), 0),
    }


rope_base = 10000000.0
norm_eps = 1e-06

def frequencies(width):
    half_width = width // 2
    exact = rope_base ** (-2.0 * np.arange(half_width) / width)
    octave = np.floor(np.log2(exact))
    quantum = 2.0 ** (8.0 - octave)
    return np.floor(exact * quantum) / quantum

def rotate(vectors, positions):
    half_width = vectors.shape[-1] // 2
    inverse = jnp.asarray(frequencies(vectors.shape[-1]), dtype=jnp.float32)
    angles = positions.astype(jnp.float32)[..., None] * inverse
    cosine = jnp.cos(angles)
    sine_part = jnp.sin(angles)
    front_half = vectors[..., :half_width]
    back_half = vectors[..., half_width:]
    return jnp.concatenate([front_half * cosine - back_half * sine_part, back_half * cosine + front_half * sine_part], axis=-1)

def arrange(columns, tp_count):
    lead = columns.shape[:-1]
    per_rank = HQ // tp_count
    query_part = columns[..., :HQ * HD].reshape(lead + (tp_count, per_rank * HD))
    key_part = jnp.repeat(columns[..., HQ * HD:(HQ + KVH) * HD].reshape(lead + (KVH, HD)), tp_count // KVH, axis=-2)
    value_part = jnp.repeat(columns[..., (HQ + KVH) * HD:].reshape(lead + (KVH, HD)), tp_count // KVH, axis=-2)
    return jnp.concatenate([query_part, key_part, value_part], axis=-1)

def reference(hidden, norm_gain, qkv_bias, qkv_weight, out_weight, key_cache, value_cache, cache_len, block_pos):
    group_size = HQ // KVH
    score_scale = HD ** (-0.5)
    hidden_wide = hidden.astype(jnp.float32)
    normed = (hidden_wide * lax.rsqrt(lax.optimization_barrier(jnp.mean(hidden_wide * hidden_wide, axis=1, keepdims=True)) + norm_eps) * norm_gain.astype(jnp.float32)).astype(jnp.bfloat16)
    joint = (jnp.dot(normed, qkv_weight, preferred_element_type=jnp.float32) + qkv_bias.astype(jnp.float32)).astype(jnp.bfloat16)
    queries = joint[:, :HQ * HD].reshape(ROLLS, HQ, HD).astype(jnp.float32)
    new_keys = joint[:, HQ * HD:(HQ + KVH) * HD].reshape(ROLLS, KVH, HD).astype(jnp.float32)
    fresh_value = joint[:, (HQ + KVH) * HD:].reshape(ROLLS, KVH, HD)
    intra_pos = (cache_len % STRETCH).astype(jnp.int32)
    fresh_key = lax.optimization_barrier(rotate(new_keys, jnp.broadcast_to(intra_pos[:, None], (ROLLS, KVH))).astype(jnp.bfloat16))
    self_query = lax.optimization_barrier(rotate(queries, jnp.broadcast_to(intra_pos[:, None], (ROLLS, HQ))).astype(jnp.bfloat16))
    block_query = lax.optimization_barrier(rotate(queries[:, None], jnp.broadcast_to(block_pos[:, :, None], (ROLLS, NBLK, HQ))).astype(jnp.bfloat16))
    self_score = score_scale * jnp.einsum('rkgd,rkd->rkg', self_query.reshape(ROLLS, KVH, group_size, HD).astype(jnp.float32), fresh_key.astype(jnp.float32))

    def one_rollout(per_rollout):
        cached_keys, cached_values, rotated_query, length, own_score, own_value = per_rollout
        keys_wide = cached_keys.reshape(NBLK, BLOCK, KVH, HD).astype(jnp.float32)
        values_wide = cached_values.reshape(NBLK, BLOCK, KVH, HD).astype(jnp.float32)
        query_wide = rotated_query.reshape(NBLK, KVH, group_size, HD).astype(jnp.float32)
        scores = score_scale * jnp.einsum('bkgd,bpkd->kgbp', query_wide, keys_wide)
        valid_mask = jnp.arange(LEN, dtype=jnp.int32).reshape(NBLK, BLOCK) < length
        masked = jnp.where(valid_mask, scores, -jnp.inf)
        top_score = jnp.maximum(lax.optimization_barrier(jnp.max(masked, axis=(2, 3))), own_score)
        weights = jnp.where(valid_mask, jnp.exp(masked - top_score[:, :, None, None]), 0.0)
        own_weight = jnp.exp(own_score - top_score)
        rounded = lax.optimization_barrier(weights.astype(jnp.bfloat16)).astype(jnp.float32)
        own_rounded = lax.optimization_barrier(own_weight.astype(jnp.bfloat16)).astype(jnp.float32)
        numerator = jnp.einsum('kgbp,bpkd->kgd', rounded, values_wide) + own_rounded[:, :, None] * own_value.astype(jnp.float32)[:, None, :]
        denominator = lax.optimization_barrier(jnp.sum(weights, axis=(2, 3))) + own_weight
        return (numerator / denominator[:, :, None]).reshape(HQ * HD).astype(jnp.bfloat16)
    attention = lax.map(one_rollout, (key_cache, value_cache, block_query, cache_len, self_score, fresh_value))
    attended = jnp.dot(attention, out_weight.T, preferred_element_type=jnp.float32).astype(jnp.bfloat16)
    fresh_kv = jnp.concatenate([fresh_key.reshape(ROLLS, KVH * HD), fresh_value.reshape(ROLLS, KVH * HD)], axis=1)
    served_qkv = arrange(qkv_weight, N_TP).reshape(D, N_TP * SCOLS)
    return (attended, fresh_kv, served_qkv, out_weight)
```

```python
import jax
import jax.numpy as jnp
import numpy as np
from jax import lax
from jax.experimental import pallas as pl
from jax.experimental.pallas import tpu as pltpu
from jax.sharding import Mesh
from jax.sharding import PartitionSpec as P

HQ = 16
KVH = 4
HD = 128
BLOCK = 512
STRETCH = 8192
PIECE = 28
COLS = 6
LINES = COLS * PIECE
TP = ("tp_0", "tp_1")
SEQ = ("seq_0", "seq_1")
SEQ_TP = ("seq_0", "seq_1", "tp_0", "tp_1")
SEQ_ROLL = ("seq_0", "seq_1", "roll")
SEQ_TP_ROLL = ("seq_0", "seq_1", "tp_0", "tp_1", "roll")

rope_base = 10000000.0
norm_eps = 1e-06
floor_score = -1e30
f32 = jnp.float32
bf16 = jnp.bfloat16


def frequencies(width):
    half_width = width // 2
    exact = rope_base ** (-2.0 * np.arange(half_width) / width)
    octave = np.floor(np.log2(exact))
    quantum = 2.0 ** (8.0 - octave)
    return np.floor(exact * quantum) / quantum


def swap(array, axes):
    return lax.all_to_all(array, axes, split_axis=0, concat_axis=0, tiled=True)


def along_x(array, step):
    place = [0, 2, 1, 3]
    return lax.ppermute(
        array, ("seq_0", "roll"), [(place[i], place[(i + step) % 4]) for i in range(4)]
    )


def along_z(array, step):
    return lax.ppermute(array, "seq_1", [(i, (i + step) % 4) for i in range(4)])


def call(kernel, outs, n_scalars, n_in, in_spaces=None, scratch=(), name=None):
    smem = pl.BlockSpec(memory_space=pltpu.SMEM)
    vmem = pl.BlockSpec(memory_space=pltpu.VMEM)
    spaces = in_spaces or [vmem] * n_in
    return pl.pallas_call(
        kernel,
        out_shape=outs,
        in_specs=[smem] * n_scalars + list(spaces),
        out_specs=jax.tree.map(lambda _: vmem, outs),
        scratch_shapes=list(scratch),
        name=name,
    )


def pack_kernel(qkv_ref, out_ref, packed_ref):
    for t in range(8):
        g = t // 2
        starts = [t * 256, t * 256 + 128, 2048 + g * 128, 2560 + g * 128]
        for c, at in enumerate(starts):
            packed_ref[t, c * PIECE : (c + 1) * PIECE, :] = qkv_ref[:, at : at + 128]
        for c in range(2):
            at = t * 256 + c * 128
            packed_ref[t, (4 + c) * PIECE : (5 + c) * PIECE, :] = out_ref[:, at : at + 128]


def expand_kernel(roll_ref, rows_ref, spread_ref):
    width = 8 * LINES
    feature = lax.broadcasted_iota(jnp.int32, (448, width), 0)
    col = lax.broadcasted_iota(jnp.int32, (448, width), 1)
    wanted = (col // LINES) * (2 * PIECE) + roll_ref[0] * PIECE + col % PIECE
    pick = jnp.where(feature == wanted, 1.0, 0.0).astype(bf16)
    spread = jnp.dot(rows_ref[...], pick, preferred_element_type=f32)
    part = lax.broadcasted_iota(jnp.int32, (8, width), 1) % LINES // PIECE
    for c in range(4):
        spread_ref[c * 8 : (c + 1) * 8, :] = jnp.where(part == c, spread, 0.0).astype(bf16)


def project_kernel(spread_ref, weight_ref, sent_ref):
    weights = weight_ref[...].reshape(8 * LINES, 128)
    sums = jnp.dot(spread_ref[...], weights, preferred_element_type=f32)
    for half in range(2):
        rows = [sums[c * 8 + half * 4 : c * 8 + half * 4 + 4] for c in range(4)]
        tile = jnp.concatenate(rows, axis=0)
        for s in range(8):
            sent_ref[s * 2 + half] = tile


def finish_kernel(parts_ref, bias_ref, sent_ref):
    total = jnp.sum(parts_ref[...], axis=0) + bias_ref[...]
    rounded = total.astype(bf16)
    for t in range(8):
        sent_ref[t] = rounded


def attend_kernel(
    scalar_ref, cols_ref, cos_ref, sin_ref, key_ref, value_ref,
    sent_ref, fresh_ref, keys, values, sems,
):
    copies = []
    for r in range(4):
        kc = pltpu.make_async_copy(key_ref.at[r], keys.at[r], sems.at[r])
        vc = pltpu.make_async_copy(value_ref.at[r], values.at[r], sems.at[4 + r])
        kc.start()
        vc.start()
        copies.append((kc, vc))
    wide = cols_ref[...].astype(f32)
    turned = pltpu.roll(wide, 64, 2)
    rotated = [
        (wide * cos_ref[b][None] + turned * sin_ref[b][None]).astype(bf16) for b in range(3)
    ]
    for g in range(4):
        fresh_ref[:, g * 128 : (g + 1) * 128] = rotated[2][2 * g, 8:12, :]
        fresh_ref[:, 512 + g * 128 : 512 + (g + 1) * 128] = cols_ref[2 * g, 12:16, :]
    row = lax.broadcasted_iota(jnp.int32, (16, 128), 0)
    col = lax.broadcasted_iota(jnp.int32, (16, 128), 1)
    group = row % 8 // 2
    spot = lax.broadcasted_iota(jnp.int32, (16, 1024), 1) + scalar_ref[4]
    flat = [rotated[b].reshape(128, 128) for b in range(2)]
    for r in range(4):
        chosen = jnp.where(col == row % 8 * 16 + row // 8 * 4 + r, 1.0, 0.0).astype(bf16)
        scores = []
        copies[r][0].wait()
        for b in range(2):
            query = jnp.dot(chosen, flat[b], preferred_element_type=f32)
            spread = jnp.concatenate(
                [jnp.where(group == g, query, 0.0) for g in range(4)], axis=1
            ).astype(bf16)
            scores.append(
                lax.dot_general(
                    spread,
                    keys[r, b * BLOCK : (b + 1) * BLOCK, :],
                    (((1,), (1,)), ((), ())),
                    preferred_element_type=f32,
                )
            )
        score = jnp.concatenate(scores, axis=1) * (HD ** (-0.5))
        valid = spot < scalar_ref[r]
        score = jnp.where(valid, score, floor_score)
        top = jnp.max(score, axis=1, keepdims=True)
        weight = jnp.where(valid, jnp.exp(score - top), 0.0)
        total = jnp.sum(weight, axis=1, keepdims=True)
        copies[r][1].wait()
        mixed = jnp.dot(weight.astype(bf16), values[r], preferred_element_type=f32)
        own = jnp.where(group == 0, mixed[:, :128], 0.0)
        for g in range(1, 4):
            own = jnp.where(group == g, mixed[:, g * 128 : (g + 1) * 128], own)
        tops = jnp.broadcast_to(top, (16, 128))
        totals = jnp.broadcast_to(total, (16, 128))
        for j in range(2):
            for t in range(8):
                at = j * 8 + t
                sent_ref[t, j * 4 + r : j * 4 + r + 1, :] = own[at : at + 1]
                sent_ref[t, 8 + j * 4 + r : 9 + j * 4 + r, :] = tops[at : at + 1]
                sent_ref[t, 16 + j * 4 + r : 17 + j * 4 + r, :] = totals[at : at + 1]


def merged(parts_ref):
    tops = [parts_ref[i, 8:16, :] for i in range(8)]
    top = tops[0]
    for other in tops[1:]:
        top = jnp.maximum(top, other)
    own = jnp.zeros((8, 128), f32)
    total = jnp.zeros((8, 128), f32)
    for i in range(8):
        factor = jnp.exp(tops[i] - top)
        own = own + parts_ref[i, 0:8, :] * factor
        total = total + parts_ref[i, 16:24, :] * factor
    return top, own, total


def merge_kernel(parts_ref, sent_ref):
    top, own, total = merged(parts_ref)
    for i in range(8):
        sent_ref[i, 0:8, :] = own
        sent_ref[i, 8:16, :] = top
        sent_ref[i, 16:24, :] = total


def assemble_kernel(
    place_ref, parts_ref, cols_ref, cos_ref, sin_ref,
    ao_ref, am_ref, ap_ref, al_ref, ah_ref, bo_ref, bm_ref, bp_ref, bl_ref, bh_ref,
    served_qkv_ref, served_out_ref, sent_ref,
):
    s0 = place_ref[0]
    z = place_ref[1]
    roll = place_ref[2]
    x = roll * 2 + s0
    other = (x + 3) % 4 // 2

    def put(low, high, s0_to, z_to, t):
        at = pl.multiple_of(((s0_to * 4 + z_to) * 8 + t) * (2 * PIECE), 8)
        for c in range(COLS):
            both = jnp.concatenate(
                [low[c * PIECE : (c + 1) * PIECE], high[c * PIECE : (c + 1) * PIECE]], axis=0
            )
            if c < 4:
                served_qkv_ref[pl.ds(at, 2 * PIECE), c * 128 : (c + 1) * 128] = both
            else:
                served_out_ref[pl.ds(at, 2 * PIECE), (c - 4) * 128 : (c - 3) * 128] = both

    def from_a(t, carry):
        for ref, dz in ((ao_ref, 0), (am_ref, 3), (ap_ref, 1)):
            z_to = (z + dz) % 4
            put(ref[roll, t], ref[1 - roll, t], s0, z_to, t)
            put(ref[2 + other, t], ref[3 - other, t], 1 - s0, z_to, t)
        z_to = (z + 2) % 4
        put(al_ref[roll, t], al_ref[1 - roll, t], s0, z_to, t)
        put(ah_ref[other, t], ah_ref[1 - other, t], 1 - s0, z_to, t)
        return carry

    lax.fori_loop(0, 4, from_a, 0)

    def from_b(own_high, minus_high):
        def step(t, carry):
            for i, dz in enumerate((0, 2, 3, 1)):
                z_to = (z + dz) % 4
                own = bo_ref[i, t]
                two = bl_ref[i, t] if i < 2 else bh_ref[i - 2, t]
                pair = (two, own) if own_high else (own, two)
                if own_high is not None:
                    put(*pair, s0, z_to, t + 4)
                if minus_high is not None:
                    minus, plus = bm_ref[i, t], bp_ref[i, t]
                    pair = (plus, minus) if minus_high else (minus, plus)
                    put(*pair, 1 - s0, z_to, t + 4)
            return carry

        lax.fori_loop(0, 4, step, 0)

    for flag in (0, 1):
        pl.when(roll == flag)(lambda flag=flag: from_b(bool(flag), None))
        pl.when(other == flag)(lambda flag=flag: from_b(None, bool(flag)))

    top, own, total = merged(parts_ref)
    wide = cols_ref[...].astype(f32)
    turned = pltpu.roll(wide, 64, 1)
    rotated = (wide * cos_ref[2] + turned * sin_ref[2]).astype(bf16).astype(f32)
    key = jnp.concatenate([rotated[8:12], rotated[8:12]], axis=0)
    self_score = jnp.sum(rotated[0:8] * key, axis=1, keepdims=True) * (HD ** (-0.5))
    self_score = jnp.broadcast_to(self_score, (8, 128))
    best = jnp.maximum(top, self_score)
    old = jnp.exp(top - best)
    fresh = jnp.exp(self_score - best)
    value = jnp.concatenate([wide[12:16], wide[12:16]], axis=0)
    numerator = own * old + fresh.astype(bf16).astype(f32) * value
    attention = numerator / (total * old + fresh)
    heads = jnp.concatenate([attention[0:4], attention[4:8]], axis=1).astype(bf16)
    partial = lax.dot_general(
        heads, served_out_ref[...], (((1,), (1,)), ((), ())), preferred_element_type=f32
    ).astype(bf16)
    for i in range(8):
        sent_ref[i] = partial


def normalize(row_block, norm_gain):
    wide_rows = row_block.astype(f32)
    scaled = wide_rows * lax.rsqrt(
        jnp.mean(wide_rows * wide_rows, axis=1, keepdims=True) + norm_eps
    )
    return (scaled * norm_gain.astype(f32)).astype(bf16)


def body(
    hidden,
    norm_gain,
    qkv_bias,
    qkv_weight,
    out_weight,
    key_cache,
    value_cache,
    cache_len,
    block_pos,
):
    tp_index = lax.axis_index(TP)
    seq_index = lax.axis_index(SEQ)
    roll_index = lax.axis_index("roll")
    shape = jax.ShapeDtypeStruct

    normed = normalize(hidden, norm_gain).reshape(4, 8, 448)
    mine = lax.dynamic_index_in_dim(normed, seq_index, 1, keepdims=False)
    theirs = lax.ppermute(mine, "roll", [(0, 1), (1, 0)])
    packed = call(pack_kernel, shape((8, LINES, 128), bf16), 0, 2, name="pack")(
        qkv_weight, out_weight
    )
    traded = swap(packed, TP)

    rows = jnp.where(
        roll_index == 0,
        jnp.concatenate([mine, theirs], axis=0),
        jnp.concatenate([theirs, mine], axis=0),
    )
    spread = call(expand_kernel, shape((32, 8 * LINES), bf16), 1, 1, name="expand")(
        roll_index.reshape(1).astype(jnp.int32), rows
    )

    a0, b0 = traded[:4], traded[4:]
    am, ap = along_x(a0, 1), along_x(a0, 3)
    bm, bp = along_z(b0, 1), along_z(b0, 3)

    sent = call(project_kernel, shape((16, 16, 128), f32), 0, 2, name="project")(spread, traded)
    parts = swap(sent, SEQ_ROLL)
    bias_wide = qkv_bias.astype(f32)
    query_bias = lax.dynamic_index_in_dim(bias_wide[:2048].reshape(8, 2, 128), tp_index, 0, False)
    key_bias = lax.dynamic_index_in_dim(bias_wide[2048:2560].reshape(4, 128), tp_index // 2, 0)
    value_bias = lax.dynamic_index_in_dim(bias_wide[2560:].reshape(4, 128), tp_index // 2, 0)
    bias = jnp.repeat(jnp.concatenate([query_bias, key_bias, value_bias], axis=0), 4, axis=0)
    copies = call(finish_kernel, shape((8, 16, 128), bf16), 0, 2, name="finish")(parts, bias)

    al, ah = along_x(am[:2], 1), along_x(ap[2:], 3)
    bl, bh = along_z(bm[:2], 1), along_z(bp[2:], 3)
    a_plane = jnp.stack([a0, jnp.concatenate([al, ah], axis=0), am, ap])
    b_plane = jnp.stack([b0, jnp.concatenate([bl, bh], axis=0), bm, bp])
    a_minus, a_plus = along_z(a_plane, 1), along_z(a_plane, 3)
    b_minus, b_plus = along_x(b_plane, 1), along_x(b_plane, 3)
    a_low, a_high = along_z(a_minus[:2], 1), along_z(a_plus[2:], 3)
    b_low, b_high = along_x(b_minus[:2], 1), along_x(b_plus[2:], 3)

    grouped = swap(copies, TP)
    inverse = np.asarray(frequencies(HD), np.float32)
    lanes = jnp.asarray(np.concatenate([inverse, inverse]))
    signs = jnp.asarray(np.concatenate([-np.ones(64), np.ones(64)]), f32)
    spots = jnp.concatenate([block_pos, (cache_len % STRETCH)[:, None]], axis=1).T
    angles = jnp.tile(spots, (1, 4)).astype(f32)[..., None] * lanes
    cosine = jnp.cos(angles)
    sine = jnp.sin(angles) * signs

    start = (seq_index * 8 + tp_index) * key_cache.shape[1]
    scalars = jnp.concatenate([cache_len, start.reshape(1).astype(jnp.int32)])
    hbm = pl.BlockSpec(memory_space=pl.ANY)
    vmem = pl.BlockSpec(memory_space=pltpu.VMEM)
    attended_parts, fresh_kv = call(
        attend_kernel,
        (shape((8, 24, 128), f32), shape((4, 1024), bf16)),
        1,
        5,
        [vmem, vmem, vmem, hbm, hbm],
        [
            pltpu.VMEM((4, 1024, 512), bf16),
            pltpu.VMEM((4, 1024, 512), bf16),
            pltpu.SemaphoreType.DMA((8,)),
        ],
        name="attend",
    )(scalars, grouped, cosine, sine, key_cache, value_cache)
    by_head = swap(attended_parts, TP)
    merged_parts = call(merge_kernel, shape((8, 24, 128), f32), 0, 1, name="merge")(by_head)
    by_place = swap(merged_parts, SEQ)

    place = jnp.stack([lax.axis_index("seq_0"), lax.axis_index("seq_1"), roll_index]).astype(jnp.int32)
    served_qkv, served_out, partial = call(
        assemble_kernel,
        (shape((3584, 512), bf16), shape((3584, 256), bf16), shape((8, 4, 3584), bf16)),
        1,
        14,
        name="assemble",
    )(
        place, by_place, copies[0], cosine, sine,
        a_plane, a_minus, a_plus, a_low, a_high, b_plane, b_minus, b_plus, b_low, b_high,
    )
    shares = swap(partial, TP)
    attended = jnp.sum(shares.astype(f32), axis=0).astype(bf16)
    return (attended, fresh_kv, served_qkv, served_out)


def solution(mesh):
    finer = Mesh(
        mesh.devices.reshape(2, 4, 4, 2, mesh.shape["roll"]),
        ("seq_0", "seq_1", "tp_0", "tp_1", "roll"),
    )
    in_specs = (
        P("roll", None),
        P(),
        P(),
        P(SEQ_TP_ROLL, None),
        P(SEQ_TP_ROLL, None),
        P("roll", SEQ_TP, None),
        P("roll", SEQ_TP, None),
        P("roll"),
        P("roll", SEQ_TP),
    )
    out_specs = (P("roll", None), P("roll", None), P(None, TP), P(None, TP))
    return jax.shard_map(body, mesh=finer, in_specs=in_specs, out_specs=out_specs, check_vma=False)
```
